8 devices in a mesh: dp: 1 (over z), row: 2 (over y), col: 4 (over x, core).
Axes of the slice: x: 2, y: 2, z: 1, core: 2. Of those that a mesh axis runs over, the one named last changes fastest.
Arguments:
- x: bfloat16 [24, 256, 6144], P(('dp', 'row'), None, 'col')
- ln_scale: float32 [6144], P('col')
- w_qkv: bfloat16 [6144, 18432], P('col', 'row')
- q_scale: float32 [128], replicated
- k_scale: float32 [128], replicated
- w_out: bfloat16 [6144, 6144], P('row', 'col')
- w_up: bfloat16 [6144, 24576], P('col', 'row')
- b_up: float32 [24576], P('row')
- w_down: bfloat16 [24576, 6144], P('row', 'col')
- b_down: float32 [6144], P('col')
Outputs:
- output: bfloat16 [24, 256, 6144], P(('dp', 'row'), None, 'col')
All inputs are finite; a program needn't handle non-finite values.
Results may differ from the reference program's by a relative error of at most 0.011318.
Values are sent between devices in bfloat16 or wider.
A program may use at most 1 GiB of HBM per device.

```python
import jax
import jax.numpy as jnp
from jax import lax

MODEL_DIM = 6144
NUM_HEADS = 48
HEAD_DIM = 128
MLP_DIM = 24576
PATCHES = 256
BATCH_PART = 24
NORM_EPS = 1e-6


def setup_inputs(seed: int = 0, part: int = 0) -> dict:
    base_key = jax.random.key(seed)
    part_keys = jax.random.split(jax.random.fold_in(base_key, part), 3)
    key_list = jax.random.split(base_key, 9)
    attn_dim = NUM_HEADS * HEAD_DIM
    width_ramp = jnp.linspace(-1.5, 1.5, MODEL_DIM)
    tok_slope = jax.random.normal(part_keys[0], (BATCH_PART, PATCHES, 1), jnp.float32)
    feat_mean = 0.5 * jax.random.normal(part_keys[1], (MODEL_DIM,), jnp.float32)
    x_noise = jax.random.normal(part_keys[2], (BATCH_PART, PATCHES, MODEL_DIM), jnp.float32)
    x = tok_slope * width_ramp + feat_mean + jnp.exp(0.3 * width_ramp) * x_noise
    ln_scale = 1.0 + 0.3 * jax.random.normal(key_list[0], (MODEL_DIM,), jnp.float32)
    branch_gain = jnp.array([3.0, 3.0, 1.0], jnp.float32).reshape(1, 1, 3, 1)
    w_qkv = jax.random.normal(key_list[1], (MODEL_DIM, NUM_HEADS, 3, HEAD_DIM), jnp.float32) * branch_gain * MODEL_DIM ** -0.5
    q_scale = 1.6 * (1.0 + 0.25 * jax.random.normal(key_list[2], (HEAD_DIM,), jnp.float32))
    k_scale = 1.6 * (1.0 + 0.25 * jax.random.normal(key_list[3], (HEAD_DIM,), jnp.float32))
    w_out = jax.random.normal(key_list[4], (attn_dim, MODEL_DIM), jnp.float32) * attn_dim ** -0.5
    w_up = jax.random.normal(key_list[5], (MODEL_DIM, MLP_DIM), jnp.float32) * MODEL_DIM ** -0.5
    b_up = 0.5 * jax.random.normal(key_list[6], (MLP_DIM,), jnp.float32)
    w_down = jax.random.normal(key_list[7], (MLP_DIM, MODEL_DIM), jnp.float32) * MLP_DIM ** -0.5
    b_down = 0.3 * jax.random.normal(key_list[8], (MODEL_DIM,), jnp.float32)
    return {
        'x': x.astype(jnp.bfloat16),
        'ln_scale': ln_scale,
        'w_qkv': w_qkv.reshape(MODEL_DIM, 3 * attn_dim).astype(jnp.bfloat16),
        'q_scale': q_scale,
        'k_scale': k_scale,
        'w_out': w_out.astype(jnp.bfloat16),
        'w_up': w_up.astype(jnp.bfloat16),
        'b_up': b_up,
        'w_down': w_down.astype(jnp.bfloat16),
        'b_down': b_down,
    }


def layer_norm_rows(values, gain_vec):
    row_mean = jnp.mean(values, axis=-1, keepdims=True)
    row_var = jnp.mean(values * values, axis=-1, keepdims=True) - row_mean * row_mean
    return (values - row_mean) * lax.rsqrt(row_var + NORM_EPS) * gain_vec


def encode_image(x_img, ln_scale, w_qkv, q_scale, k_scale, w_out, w_up, b_up, w_down, b_down):
    x_f32 = x_img.astype(jnp.float32)
    normed = layer_norm_rows(x_f32, ln_scale).astype(jnp.bfloat16)
    qkv_proj = jnp.dot(normed, w_qkv, preferred_element_type=jnp.float32).astype(jnp.bfloat16)
    qkv_heads = qkv_proj.astype(jnp.float32).reshape(PATCHES, NUM_HEADS, 3, HEAD_DIM)
    q_normed = layer_norm_rows(qkv_heads[:, :, 0], q_scale).astype(jnp.bfloat16).astype(jnp.float32)
    k_normed = layer_norm_rows(qkv_heads[:, :, 1], k_scale).astype(jnp.bfloat16).astype(jnp.float32)
    v_heads = qkv_heads[:, :, 2]
    scores = jnp.einsum('shd,thd->hst', q_normed, k_normed) * HEAD_DIM ** -0.5
    attn_prob = jax.nn.softmax(scores, axis=-1).astype(jnp.bfloat16).astype(jnp.float32)
    attn_out = jnp.einsum('hst,thd->shd', attn_prob, v_heads).astype(jnp.bfloat16).reshape(PATCHES, NUM_HEADS * HEAD_DIM)
    up_proj = jnp.dot(normed, w_up, preferred_element_type=jnp.float32).astype(jnp.bfloat16)
    gelu_out = jax.nn.gelu(up_proj.astype(jnp.float32) + b_up, approximate=True).astype(jnp.bfloat16)
    branch_sum = jnp.dot(attn_out, w_out, preferred_element_type=jnp.float32) + jnp.dot(gelu_out, w_down, preferred_element_type=jnp.float32)
    return (x_f32 + branch_sum + b_down).astype(jnp.bfloat16)


def reference(x, ln_scale, w_qkv, q_scale, k_scale, w_out, w_up, b_up, w_down, b_down):
    return lax.map(lambda x_img: encode_image(x_img, ln_scale, w_qkv, q_scale, k_scale, w_out, w_up, b_up, w_down, b_down), x)
```

```python
import functools
import jax
import jax.numpy as jnp
from jax import lax
from jax.experimental import pallas as pl
from jax.experimental.pallas import tpu as pltpu
from jax.sharding import PartitionSpec as P


NORM_EPS = 1e-6
VMEM_LIMIT = 60 * 1024 * 1024
UP_PIECES = 4
OUT_PIECES = (512, 512, 256, 256)
Y_PIECES = 4


def layer_norm_rows(values, gain_vec):
    row_mean = jnp.mean(values, axis=-1, keepdims=True)
    row_var = jnp.mean(values * values, axis=-1, keepdims=True) - row_mean * row_mean
    return (values - row_mean) * lax.rsqrt(row_var + NORM_EPS) * gain_vec


def tile_of(size, want):
    tile = min(size, want)
    while size % tile:
        tile //= 2
    return tile


def normalise_tile(n_blocks, *refs):
    x_refs, gain_refs, out_refs = refs[:n_blocks], refs[n_blocks:2 * n_blocks], refs[2 * n_blocks:]
    full_width = n_blocks * x_refs[0].shape[1]
    total, squares = 0.0, 0.0
    for x_ref in x_refs:
        values = x_ref[...].astype(jnp.float32)
        total = total + jnp.sum(values, axis=-1, keepdims=True)
        squares = squares + jnp.sum(values * values, axis=-1, keepdims=True)
    row_mean = total / full_width
    row_var = squares / full_width - row_mean * row_mean
    inv = lax.rsqrt(row_var + NORM_EPS)
    for x_ref, gain_ref, out_ref in zip(x_refs, gain_refs, out_refs):
        out_ref[...] = ((x_ref[...].astype(jnp.float32) - row_mean) * inv * gain_ref[...]).astype(jnp.bfloat16)


def normalise(x_list, gain_list):
    rows, depth = x_list[0].shape
    n_blocks = len(x_list)
    bm = tile_of(rows, 256)
    row_block = pl.BlockSpec((bm, depth), lambda i: (i, 0))
    return pl.pallas_call(
        functools.partial(normalise_tile, n_blocks),
        out_shape=[jax.ShapeDtypeStruct((rows, depth), jnp.bfloat16)] * n_blocks,
        grid=(rows // bm,),
        in_specs=[row_block] * n_blocks + [pl.BlockSpec((1, depth), lambda i: (0, 0))] * n_blocks,
        out_specs=[row_block] * n_blocks,
        compiler_params=pltpu.CompilerParams(vmem_limit_bytes=VMEM_LIMIT),
        cost_estimate=pl.CostEstimate(flops=600 * rows * depth * n_blocks, bytes_accessed=4 * rows * depth * n_blocks, transcendentals=0),
    )(*x_list, *[g.reshape(1, depth) for g in gain_list])


def block_matmul(n_blocks, with_gelu, *refs):
    n_refs, w_refs = refs[:n_blocks], refs[n_blocks:2 * n_blocks]
    out_ref = refs[-1]
    acc = jnp.dot(n_refs[0][...], w_refs[0][...], preferred_element_type=jnp.float32)
    for n_ref, w_ref in zip(n_refs[1:], w_refs[1:]):
        acc = acc + jnp.dot(n_ref[...], w_ref[...], preferred_element_type=jnp.float32)
    out = acc.astype(jnp.bfloat16)
    if with_gelu:
        bias_ref = refs[2 * n_blocks]
        out = jax.nn.gelu(out.astype(jnp.float32) + bias_ref[...], approximate=True).astype(jnp.bfloat16)
    out_ref[...] = out


def project_in(n_list, w_list, bias):
    rows, depth = n_list[0].shape
    cols = w_list[0].shape[1]
    n_blocks = len(n_list)
    bm, bn = tile_of(rows, 512), 768 if cols % 768 == 0 else tile_of(cols, 512)
    in_specs = [pl.BlockSpec((bm, depth), lambda j, i: (i, 0))] * n_blocks
    in_specs += [pl.BlockSpec((depth, bn), lambda j, i: (0, j))] * n_blocks
    operands = [*n_list, *w_list]
    if bias is not None:
        in_specs.append(pl.BlockSpec((1, bn), lambda j, i: (0, j)))
        operands.append(bias.reshape(1, cols))
    flops = 2 * rows * depth * n_blocks * cols
    return pl.pallas_call(
        functools.partial(block_matmul, n_blocks, bias is not None),
        out_shape=jax.ShapeDtypeStruct((rows, cols), jnp.bfloat16),
        grid=(cols // bn, rows // bm),
        in_specs=in_specs,
        out_specs=pl.BlockSpec((bm, bn), lambda j, i: (i, j)),
        compiler_params=pltpu.CompilerParams(vmem_limit_bytes=VMEM_LIMIT),
        cost_estimate=pl.CostEstimate(flops=flops, bytes_accessed=4 * n_blocks * depth * (rows + cols), transcendentals=0),
    )(*operands)


def out_matmul(n_hidden, n_adds, n_parts, has_res, *refs):
    out_ref = refs[-1]
    hidden_refs, w_ref = refs[:n_hidden], refs[n_hidden]
    rest = refs[n_hidden + 1:-1]
    acc, start = None, 0
    for h_ref in hidden_refs:
        stop = start + h_ref.shape[1]
        term = jnp.dot(h_ref[...], w_ref[start:stop], preferred_element_type=jnp.float32)
        acc = term if acc is None else acc + term
        start = stop
    for add_ref in rest[:n_adds]:
        acc = acc + add_ref[...].astype(jnp.float32)
    rest = rest[n_adds:]
    if has_res:
        acc = rest[n_parts][...].astype(jnp.float32) + acc + rest[n_parts + 1][...]
    if not n_parts:
        out_ref[...] = acc.astype(out_ref.dtype)
    start = 0
    for part_ref in rest[:n_parts]:
        stop = start + part_ref.shape[1]
        out_ref[:, start:stop] = (acc[:, start:stop] + part_ref[...].astype(jnp.float32)).astype(out_ref.dtype)
        start = stop


def project_out(hidden, w, adds, parts=(), residual=None, bias=None, window=(0, 1)):
    rows = hidden[0].shape[0]
    index, count = window
    depth, cols = w.shape[0], w.shape[1] // count
    bm = tile_of(rows, 512)
    row_block = lambda width: pl.BlockSpec((bm, width), lambda i: (i, 0))
    in_specs = [row_block(h.shape[1]) for h in hidden] + [pl.BlockSpec((depth, cols), lambda i: (0, index))]
    in_specs += [pl.BlockSpec((bm, cols), lambda i: (i, index))] * len(adds)
    in_specs += [row_block(p.shape[1]) for p in parts]
    operands = [*hidden, w, *adds, *parts]
    out_type = jnp.bfloat16
    if residual is not None:
        in_specs += [row_block(cols), pl.BlockSpec((1, cols), lambda i: (0, 0))]
        operands += [residual, bias.reshape(1, cols)]
        out_type = jnp.float32
    return pl.pallas_call(
        functools.partial(out_matmul, len(hidden), len(adds), len(parts), residual is not None),
        out_shape=jax.ShapeDtypeStruct((rows, cols), out_type),
        grid=(rows // bm,),
        in_specs=in_specs,
        out_specs=row_block(cols),
        compiler_params=pltpu.CompilerParams(vmem_limit_bytes=VMEM_LIMIT),
        cost_estimate=pl.CostEstimate(flops=2 * rows * depth * cols, bytes_accessed=2 * (rows + cols) * depth, transcendentals=0),
    )(*operands)


def add_parts(main_ref, *refs):
    out_ref, start = refs[-1], 0
    for part_ref in refs[:-1]:
        stop = start + part_ref.shape[1]
        out_ref[:, start:stop] = (main_ref[:, start:stop] + part_ref[...].astype(jnp.float32)).astype(out_ref.dtype)
        start = stop


def add_last(main_ref, part_ref, held_ref, out_ref):
    out_ref[...] = (main_ref[...] + part_ref[...].astype(jnp.float32)).astype(out_ref.dtype)


def join_parts(main, parts):
    rows, cols = main.shape
    bm = tile_of(rows, 512)
    row_block = lambda width: pl.BlockSpec((bm, width), lambda i: (i, 0))
    return pl.pallas_call(
        add_parts,
        out_shape=jax.ShapeDtypeStruct((rows, cols), jnp.bfloat16),
        grid=(rows // bm,),
        in_specs=[row_block(cols)] + [row_block(p.shape[1]) for p in parts],
        out_specs=row_block(cols),
        compiler_params=pltpu.CompilerParams(vmem_limit_bytes=VMEM_LIMIT),
        cost_estimate=pl.CostEstimate(flops=2 * rows * cols, bytes_accessed=8 * rows * cols, transcendentals=0),
    )(main, *parts)


def join_last(main, part, held):
    rows, cols = main.shape
    size = part.shape[1]
    bm = tile_of(rows, 1024)
    last = cols // size - 1
    tail_block = pl.BlockSpec((bm, size), lambda i: (i, last))
    return pl.pallas_call(
        add_last,
        out_shape=jax.ShapeDtypeStruct((rows, cols), jnp.bfloat16),
        grid=(rows // bm,),
        in_specs=[tail_block, pl.BlockSpec((bm, size), lambda i: (i, 0)), pl.BlockSpec(memory_space=pl.ANY)],
        out_specs=tail_block,
        input_output_aliases={2: 0},
        compiler_params=pltpu.CompilerParams(vmem_limit_bytes=VMEM_LIMIT),
        cost_estimate=pl.CostEstimate(flops=2 * rows * size, bytes_accessed=8 * rows * size, transcendentals=0),
    )(main, part, held)


def attend(head_dim, qs_ref, ks_ref, *refs):
    out_ref, done = refs[-1], 0
    for qkv_ref in refs[:-1]:
        for base in range(0, qkv_ref.shape[1], 3 * head_dim):
            q = layer_norm_rows(qkv_ref[:, base:base + head_dim].astype(jnp.float32), qs_ref[...]).astype(jnp.bfloat16)
            k = layer_norm_rows(qkv_ref[:, base + head_dim:base + 2 * head_dim].astype(jnp.float32), ks_ref[...]).astype(jnp.bfloat16)
            v = qkv_ref[:, base + 2 * head_dim:base + 3 * head_dim]
            s = lax.dot_general(q, k, (((1,), (1,)), ((), ())), preferred_element_type=jnp.float32) * head_dim ** -0.5
            e = jnp.exp(s - jnp.max(s, axis=-1, keepdims=True))
            p = (e / jnp.sum(e, axis=-1, keepdims=True)).astype(jnp.bfloat16)
            out_ref[:, done:done + head_dim] = jnp.dot(p, v, preferred_element_type=jnp.float32).astype(jnp.bfloat16)
            done += head_dim


def attention(qkv_list, q_scale, k_scale, seq_len):
    rows = qkv_list[0].shape[0]
    widths = [q.shape[1] for q in qkv_list]
    head_dim = q_scale.shape[0]
    out_width = sum(widths) // 3
    scale_spec = pl.BlockSpec((1, head_dim), lambda i: (0, 0))
    flops = 4 * rows * seq_len * out_width
    return pl.pallas_call(
        functools.partial(attend, head_dim),
        out_shape=jax.ShapeDtypeStruct((rows, out_width), jnp.bfloat16),
        grid=(rows // seq_len,),
        in_specs=[scale_spec, scale_spec] + [pl.BlockSpec((seq_len, w), lambda i: (i, 0)) for w in widths],
        out_specs=pl.BlockSpec((seq_len, out_width), lambda i: (i, 0)),
        compiler_params=pltpu.CompilerParams(vmem_limit_bytes=VMEM_LIMIT),
        cost_estimate=pl.CostEstimate(flops=8 * flops, bytes_accessed=2 * rows * sum(widths), transcendentals=0),
    )(q_scale.reshape(1, head_dim), k_scale.reshape(1, head_dim), *qkv_list)


def solution(mesh):
    col_size = mesh.shape['col']
    row_size = mesh.shape['row']

    def partner(arr, shift):
        return lax.ppermute(arr, 'col', [(i, i ^ shift) for i in range(col_size)])

    def over_row(arr):
        return lax.ppermute(arr, 'row', [(i, i ^ 1) for i in range(row_size)])

    def layer(x_loc, ln_scale, w_qkv, q_scale, k_scale, w_out, w_up, b_up, w_down, b_down):
        col = lax.axis_index('col')
        imgs, seq_len, width = x_loc.shape
        x_rows = x_loc.reshape(imgs * seq_len, width)

        def piece_cols(w, shift, start, size):
            span = w.shape[1] // col_size
            return lax.dynamic_slice(w, (0, (col ^ shift) * span + start), (w.shape[0], size))

        def piece_rows(w, shift, start, size):
            span = w.shape[0] // col_size
            return lax.dynamic_slice(w, ((col ^ shift) * span, start), (span, size))

        def in_weights(w, start, size):
            return [piece_cols(w, 0, start, size)] + [
                partner(piece_cols(w, s, start, size), s) for s in (1, 2, 3)]

        def out_piece(shift, start, size):
            return jnp.concatenate([piece_rows(w_out, shift, start, size), piece_rows(w_down, shift, start, size)], axis=0)

        gains = [ln_scale] + [partner(ln_scale, s) for s in (1, 2, 3)]
        x1 = partner(x_rows, 1)
        x2 = partner(x_rows, 2)
        z0 = over_row(x_rows)
        x3 = partner(x2, 1)
        z2 = over_row(x2)
        z1 = partner(z0, 1)
        z3 = partner(z2, 1)
        own = normalise([x_rows, x1, x2, x3], gains)
        oth = normalise([z0, z1, z2, z3], gains)

        head_cols = 3 * q_scale.shape[0]
        qkv_cols = w_qkv.shape[1] // col_size
        up_cols = w_up.shape[1] // col_size
        qkv_step, up_step = 2 * head_cols, up_cols // UP_PIECES
        qkv_own, qkv_oth, g_own, g_oth = [], [], [], []
        for i in range(qkv_cols // qkv_step):
            w = in_weights(w_qkv, i * qkv_step, qkv_step)
            qkv_own.append(project_in(own, w, None))
            qkv_oth.append(project_in(oth, w, None))
        attn_own = attention(qkv_own, q_scale, k_scale, seq_len)
        attn_oth = attention(qkv_oth, q_scale, k_scale, seq_len)
        for i in range(UP_PIECES):
            w = in_weights(w_up, i * up_step, up_step)
            bias = lax.dynamic_slice(b_up, (col * up_cols + i * up_step,), (up_step,))
            g_own.append(project_in(own, w, bias))
            g_oth.append(project_in(oth, w, bias))
        hid_own, hid_oth = [attn_own, *g_own], [attn_oth, *g_oth]

        out_cols = w_out.shape[1]
        wo_0 = out_piece(0, 0, out_cols)
        wo_1 = partner(out_piece(1, 0, out_cols), 1)
        d1_oth = partner(project_out(hid_oth, wo_1, []), 1)
        d1_own = partner(project_out(hid_own, wo_1, []), 1)
        y0 = [over_row(project_out(hid_oth, wo_0, [d1_oth], window=(i, Y_PIECES))) for i in range(Y_PIECES)]
        x_parts, start = [], 0
        for size in OUT_PIECES:
            wo_3 = partner(out_piece(3, start, size), 3)
            wo_2 = partner(out_piece(2, start, size), 2)
            d3_oth = partner(project_out(hid_oth, wo_3, []), 1)
            d3_own = partner(project_out(hid_own, wo_3, []), 1)
            y2 = over_row(project_out(hid_oth, wo_2, [d3_oth]))
            x_parts.append(partner(project_out(hid_own, wo_2, [d3_own, y2]), 2))
            start += size
        main = project_out(hid_own, wo_0, [d1_own], parts=y0, residual=x_rows, bias=b_down)
        out = join_last(main, x_parts[-1], join_parts(main, x_parts[:-1]))
        return out.reshape(imgs, seq_len, width)

    x_spec = P(('dp', 'row'), None, 'col')
    return jax.shard_map(layer, mesh=mesh,
                         in_specs=(x_spec, P('col'), P('col', 'row'), P(), P(), P('row', 'col'), P('col', 'row'), P('row'), P('row', 'col'), P('col')),
                         out_specs=x_spec, check_vma=False)
```

```python
import functools
import jax
import jax.numpy as jnp
from jax import lax
from jax.experimental import pallas as pl
from jax.experimental.pallas import tpu as pltpu
from jax.sharding import PartitionSpec as P


NORM_EPS = 1e-6
VMEM_LIMIT = 60 * 1024 * 1024
UP_PIECES = 4
OUT_PIECES = (512, 512, 256, 256)
Y_PIECES = 3
EARLY = 2


def layer_norm_rows(values, gain_vec):
    row_mean = jnp.mean(values, axis=-1, keepdims=True)
    row_var = jnp.mean(values * values, axis=-1, keepdims=True) - row_mean * row_mean
    return (values - row_mean) * lax.rsqrt(row_var + NORM_EPS) * gain_vec


def tile_of(size, want):
    tile = min(size, want)
    while size % tile:
        tile //= 2
    return tile


def normalise_tile(n_blocks, *refs):
    x_refs, gain_refs, out_refs = refs[:n_blocks], refs[n_blocks:2 * n_blocks], refs[-n_blocks:]
    full_width = n_blocks * x_refs[0].shape[1]
    total, squares = 0.0, 0.0
    for x_ref in x_refs:
        values = x_ref[...].astype(jnp.float32)
        total = total + jnp.sum(values, axis=-1, keepdims=True)
        squares = squares + jnp.sum(values * values, axis=-1, keepdims=True)
    row_mean = total / full_width
    row_var = squares / full_width - row_mean * row_mean
    inv = lax.rsqrt(row_var + NORM_EPS)
    for x_ref, gain_ref, out_ref in zip(x_refs, gain_refs, out_refs):
        out_ref[...] = ((x_ref[...].astype(jnp.float32) - row_mean) * inv * gain_ref[...]).astype(jnp.bfloat16)


def normalise(x_list, gain_list, held):
    rows, depth = x_list[0].shape
    n_blocks = len(x_list)
    bm = tile_of(rows, 64)
    steps = rows // bm
    shift = steps if held else 0
    row_block = pl.BlockSpec((bm, depth), lambda i: (i, 0))
    held = list(held or [])
    return pl.pallas_call(
        functools.partial(normalise_tile, n_blocks),
        out_shape=[jax.ShapeDtypeStruct((2 * rows, depth), jnp.bfloat16)] * n_blocks,
        grid=(steps,),
        in_specs=[row_block] * n_blocks + [pl.BlockSpec((1, depth), lambda i: (0, 0))] * n_blocks
        + [pl.BlockSpec(memory_space=pl.ANY)] * len(held),
        out_specs=[pl.BlockSpec((bm, depth), lambda i: (i + shift, 0))] * n_blocks,
        input_output_aliases={2 * n_blocks + k: k for k in range(len(held))},
        compiler_params=pltpu.CompilerParams(vmem_limit_bytes=VMEM_LIMIT),
        cost_estimate=pl.CostEstimate(flops=600 * rows * depth * n_blocks, bytes_accessed=4 * rows * depth * n_blocks, transcendentals=0),
    )(*x_list, *[g.reshape(1, depth) for g in gain_list], *held)


def lane_tile(cols):
    return 256 if cols % 256 == 0 else 128


def block_matmul(n_blocks, with_gelu, *refs):
    n_refs, w_refs = refs[:n_blocks], refs[n_blocks:2 * n_blocks]
    out_ref = refs[-1]
    tile = lane_tile(out_ref.shape[1])

    def step(t, carry):
        cols = pl.ds(pl.multiple_of(t * tile, tile), tile)
        acc = jnp.dot(n_refs[0][...], w_refs[0][:, cols], preferred_element_type=jnp.float32)
        for n_ref, w_ref in zip(n_refs[1:], w_refs[1:]):
            acc = acc + jnp.dot(n_ref[...], w_ref[:, cols], preferred_element_type=jnp.float32)
        out = acc.astype(jnp.bfloat16)
        if with_gelu:
            bias = refs[2 * n_blocks][:, cols]
            out = jax.nn.gelu(out.astype(jnp.float32) + bias, approximate=True).astype(jnp.bfloat16)
        out_ref[:, cols] = out
        return carry

    lax.fori_loop(0, out_ref.shape[1] // tile, step, 0)


def project_in(n_list, w_list, bias, half=None, held=None):
    rows, depth = n_list[0].shape
    cols = w_list[0].shape[1]
    n_blocks = len(n_list)
    bm, bn = tile_of(rows // 2, 256), 768 if cols % 768 == 0 else tile_of(cols, 512)
    steps = rows // bm if half is None else rows // bm // 2
    shift = steps if half else 0
    in_specs = [pl.BlockSpec((bm, depth), lambda j, i: (i + shift, 0))] * n_blocks
    in_specs += [pl.BlockSpec((depth, bn), lambda j, i: (0, j))] * n_blocks
    operands = [*n_list, *w_list]
    if bias is not None:
        in_specs.append(pl.BlockSpec((1, bn), lambda j, i: (0, j)))
        operands.append(bias.reshape(1, cols))
    aliases = {}
    if held is not None:
        in_specs.append(pl.BlockSpec(memory_space=pl.ANY))
        aliases = {len(operands): 0}
        operands.append(held)
    flops = 2 * bm * steps * depth * n_blocks * cols
    return pl.pallas_call(
        functools.partial(block_matmul, n_blocks, bias is not None),
        out_shape=jax.ShapeDtypeStruct((rows, cols), jnp.bfloat16),
        grid=(cols // bn, steps),
        in_specs=in_specs,
        out_specs=pl.BlockSpec((bm, bn), lambda j, i: (i + shift, j)),
        input_output_aliases=aliases,
        compiler_params=pltpu.CompilerParams(vmem_limit_bytes=VMEM_LIMIT),
        cost_estimate=pl.CostEstimate(flops=flops, bytes_accessed=4 * n_blocks * depth * (rows + cols), transcendentals=0),
    )(*operands)


def out_matmul(n_hidden, n_adds, n_parts, has_res, *refs):
    out_ref = refs[-1]
    hidden_refs, w_ref = refs[:n_hidden], refs[n_hidden]
    rest = refs[n_hidden + 1:-1]
    tile = lane_tile(out_ref.shape[1])

    def step(t, carry):
        cols = pl.ds(pl.multiple_of(t * tile, tile), tile)
        acc, start = None, 0
        for h_ref in hidden_refs:
            stop = start + h_ref.shape[1]
            term = jnp.dot(h_ref[...], w_ref[start:stop, cols], preferred_element_type=jnp.float32)
            acc = term if acc is None else acc + term
            start = stop
        for add_ref in rest[:n_adds]:
            acc = acc + add_ref[:, cols].astype(jnp.float32)
        if has_res:
            acc = rest[n_adds + n_parts][:, cols].astype(jnp.float32) + acc + rest[n_adds + n_parts + 1][:, cols]
        out_ref[:, cols] = acc.astype(out_ref.dtype)
        return carry

    lax.fori_loop(0, out_ref.shape[1] // tile, step, 0)
    start = 0
    for part_ref in rest[n_adds:n_adds + n_parts]:
        stop = start + part_ref.shape[1]
        out_ref[:, start:stop] = out_ref[:, start:stop] + part_ref[...].astype(jnp.float32)
        start = stop


def project_out(hidden, w, adds, half=None, parts=(), residual=None, bias=None, window=(0, 1)):
    all_rows = hidden[0].shape[0]
    rows = all_rows if half is None else all_rows // 2
    index, count = window
    depth, cols = w.shape[0], w.shape[1] // count
    bm = tile_of(rows, 512)

    def row_block(arr, width, col_index=0):
        shift = rows // bm if half and arr.shape[0] == all_rows else 0
        return pl.BlockSpec((bm, width), lambda i: (i + shift, col_index))

    in_specs = [row_block(h, h.shape[1]) for h in hidden] + [pl.BlockSpec((depth, cols), lambda i: (0, index))]
    in_specs += [row_block(a, cols, index) for a in adds]
    in_specs += [row_block(p, p.shape[1]) for p in parts]
    operands = [*hidden, w, *adds, *parts]
    out_type = jnp.bfloat16
    if residual is not None:
        in_specs += [row_block(residual, cols), pl.BlockSpec((1, cols), lambda i: (0, 0))]
        operands += [residual, bias.reshape(1, cols)]
        out_type = jnp.float32
    return pl.pallas_call(
        functools.partial(out_matmul, len(hidden), len(adds), len(parts), residual is not None),
        out_shape=jax.ShapeDtypeStruct((rows, cols), out_type),
        grid=(rows // bm,),
        in_specs=in_specs,
        out_specs=pl.BlockSpec((bm, cols), lambda i: (i, 0)),
        compiler_params=pltpu.CompilerParams(vmem_limit_bytes=VMEM_LIMIT),
        cost_estimate=pl.CostEstimate(flops=2 * rows * depth * cols, bytes_accessed=2 * (rows + cols) * depth, transcendentals=0),
    )(*operands)


def add_parts(main_ref, *refs):
    out_ref, start = refs[-1], 0
    for part_ref in refs[:-1]:
        stop = start + part_ref.shape[1]
        out_ref[:, start:stop] = (main_ref[:, start:stop] + part_ref[...].astype(jnp.float32)).astype(out_ref.dtype)
        start = stop


def add_last(main_ref, part_ref, held_ref, out_ref):
    out_ref[...] = (main_ref[...] + part_ref[...].astype(jnp.float32)).astype(out_ref.dtype)


def join_parts(main, parts):
    rows, cols = main.shape
    bm = tile_of(rows, 128)
    row_block = lambda width: pl.BlockSpec((bm, width), lambda i: (i, 0))
    return pl.pallas_call(
        add_parts,
        out_shape=jax.ShapeDtypeStruct((rows, cols), jnp.bfloat16),
        grid=(rows // bm,),
        in_specs=[row_block(cols)] + [row_block(p.shape[1]) for p in parts],
        out_specs=row_block(cols),
        compiler_params=pltpu.CompilerParams(vmem_limit_bytes=VMEM_LIMIT),
        cost_estimate=pl.CostEstimate(flops=2 * rows * cols, bytes_accessed=8 * rows * cols, transcendentals=0),
    )(main, *parts)


def join_last(main, part, held):
    rows, cols = main.shape
    size = part.shape[1]
    bm = tile_of(rows, 1024)
    last = cols // size - 1
    tail_block = pl.BlockSpec((bm, size), lambda i: (i, last))
    return pl.pallas_call(
        add_last,
        out_shape=jax.ShapeDtypeStruct((rows, cols), jnp.bfloat16),
        grid=(rows // bm,),
        in_specs=[tail_block, pl.BlockSpec((bm, size), lambda i: (i, 0)), pl.BlockSpec(memory_space=pl.ANY)],
        out_specs=tail_block,
        input_output_aliases={2: 0},
        compiler_params=pltpu.CompilerParams(vmem_limit_bytes=VMEM_LIMIT),
        cost_estimate=pl.CostEstimate(flops=2 * rows * size, bytes_accessed=8 * rows * size, transcendentals=0),
    )(main, part, held)


def attend(head_dim, qs_ref, ks_ref, *refs):
    out_ref, done = refs[-1], 0
    for qkv_ref in refs[:-1]:
        for base in range(0, qkv_ref.shape[1], 3 * head_dim):
            q = layer_norm_rows(qkv_ref[:, base:base + head_dim].astype(jnp.float32), qs_ref[...]).astype(jnp.bfloat16)
            k = layer_norm_rows(qkv_ref[:, base + head_dim:base + 2 * head_dim].astype(jnp.float32), ks_ref[...]).astype(jnp.bfloat16)
            v = qkv_ref[:, base + 2 * head_dim:base + 3 * head_dim]
            s = lax.dot_general(q, k, (((1,), (1,)), ((), ())), preferred_element_type=jnp.float32) * head_dim ** -0.5
            e = jnp.exp(s - jnp.max(s, axis=-1, keepdims=True))
            p = (e / jnp.sum(e, axis=-1, keepdims=True)).astype(jnp.bfloat16)
            out_ref[:, done:done + head_dim] = jnp.dot(p, v, preferred_element_type=jnp.float32).astype(jnp.bfloat16)
            done += head_dim


def attention(qkv_list, q_scale, k_scale, seq_len):
    rows = qkv_list[0].shape[0]
    widths = [q.shape[1] for q in qkv_list]
    head_dim = q_scale.shape[0]
    out_width = sum(widths) // 3
    scale_spec = pl.BlockSpec((1, head_dim), lambda i: (0, 0))
    flops = 4 * rows * seq_len * out_width
    return pl.pallas_call(
        functools.partial(attend, head_dim),
        out_shape=jax.ShapeDtypeStruct((rows, out_width), jnp.bfloat16),
        grid=(rows // seq_len,),
        in_specs=[scale_spec, scale_spec] + [pl.BlockSpec((seq_len, w), lambda i: (i, 0)) for w in widths],
        out_specs=pl.BlockSpec((seq_len, out_width), lambda i: (i, 0)),
        compiler_params=pltpu.CompilerParams(vmem_limit_bytes=VMEM_LIMIT),
        cost_estimate=pl.CostEstimate(flops=8 * flops, bytes_accessed=2 * rows * sum(widths), transcendentals=0),
    )(q_scale.reshape(1, head_dim), k_scale.reshape(1, head_dim), *qkv_list)


def solution(mesh):
    col_size = mesh.shape['col']
    row_size = mesh.shape['row']

    def partner(arr, shift):
        return lax.ppermute(arr, 'col', [(i, i ^ shift) for i in range(col_size)])

    def over_row(arr):
        return lax.ppermute(arr, 'row', [(i, i ^ 1) for i in range(row_size)])

    def layer(x_loc, ln_scale, w_qkv, q_scale, k_scale, w_out, w_up, b_up, w_down, b_down):
        col = lax.axis_index('col')
        imgs, seq_len, width = x_loc.shape
        x_rows = x_loc.reshape(imgs * seq_len, width)

        def piece_cols(w, shift, start, size):
            span = w.shape[1] // col_size
            return lax.dynamic_slice(w, (0, (col ^ shift) * span + start), (w.shape[0], size))

        def piece_rows(w, shift, start, size):
            span = w.shape[0] // col_size
            return lax.dynamic_slice(w, ((col ^ shift) * span, start), (span, size))

        def in_weights(w, start, size):
            return [piece_cols(w, 0, start, size)] + [
                partner(piece_cols(w, s, start, size), s) for s in (1, 2, 3)]

        def out_piece(shift, start, size):
            return jnp.concatenate([piece_rows(w_out, shift, start, size), piece_rows(w_down, shift, start, size)], axis=0)

        gains = [ln_scale] + [partner(ln_scale, s) for s in (1, 2, 3)]
        x1 = partner(x_rows, 1)
        x2 = partner(x_rows, 2)
        z0 = over_row(x_rows)
        x3 = partner(x2, 1)
        z2 = over_row(x2)
        z1 = partner(z0, 1)
        z3 = partner(z2, 1)
        first = normalise([x_rows, x1, x2, x3], gains, None)
        both = normalise([z0, z1, z2, z3], gains, first)

        head_cols = 3 * q_scale.shape[0]
        qkv_cols = w_qkv.shape[1] // col_size
        up_cols = w_up.shape[1] // col_size
        qkv_step, up_step = 2 * head_cols, up_cols // UP_PIECES
        qkv, hidden = [], []
        for i in range(qkv_cols // qkv_step):
            w = in_weights(w_qkv, i * qkv_step, qkv_step)
            if i < EARLY:
                part = project_in(first, w, None, half=0)
                qkv.append(project_in(both, w, None, half=1, held=part))
            else:
                qkv.append(project_in(both, w, None))
        hidden.append(attention(qkv, q_scale, k_scale, seq_len))
        for i in range(UP_PIECES):
            w = in_weights(w_up, i * up_step, up_step)
            bias = lax.dynamic_slice(b_up, (col * up_cols + i * up_step,), (up_step,))
            if i < UP_PIECES - 1:
                hidden.append(project_in(both, w, bias))
        up_oth = project_in(both, w, bias, half=1)
        up_both = project_in(both, w, bias, half=0, held=up_oth)
        hid_oth, hid = [*hidden, up_oth], [*hidden, up_both]

        out_cols = w_out.shape[1]
        wo_0 = out_piece(0, 0, out_cols)
        wo_1 = partner(out_piece(1, 0, out_cols), 1)
        d1_oth = partner(project_out(hid_oth, wo_1, [], half=1), 1)
        d1_own = partner(project_out(hid, wo_1, [], half=0), 1)
        y0 = [over_row(project_out(hid, wo_0, [d1_oth], half=1, window=(i, Y_PIECES))) for i in range(Y_PIECES)]
        x_parts, start = [], 0
        for size in OUT_PIECES:
            wo_3 = partner(out_piece(3, start, size), 3)
            wo_2 = partner(out_piece(2, start, size), 2)
            d3 = partner(project_out(hid, wo_3, []), 1)
            y2 = over_row(project_out(hid, wo_2, [d3], half=1))
            x_parts.append(partner(project_out(hid, wo_2, [d3, y2], half=0), 2))
            start += size
        main = project_out(hid, wo_0, [d1_own], half=0, parts=y0, residual=x_rows, bias=b_down)
        out = join_last(main, x_parts[-1], join_parts(main, x_parts[:-1]))
        return out.reshape(imgs, seq_len, width)

    x_spec = P(('dp', 'row'), None, 'col')
    return jax.shard_map(layer, mesh=mesh,
                         in_specs=(x_spec, P('col'), P('col', 'row'), P(), P(), P('row', 'col'), P('col', 'row'), P('row'), P('row', 'col'), P('col')),
                         out_specs=x_spec, check_vma=False)
```

```python
import functools
import jax
import jax.numpy as jnp
from jax import lax
from jax.experimental import pallas as pl
from jax.experimental.pallas import tpu as pltpu
from jax.sharding import PartitionSpec as P


NORM_EPS = 1e-6
VMEM_LIMIT = 60 * 1024 * 1024
SMALL_LIMIT = 16 * 1024 * 1024
UP_PIECES = 4
OUT_PIECES = (512, 512, 256, 256)
Y_PIECES = 3
EARLY = 2


def layer_norm_rows(values, gain_vec):
    row_mean = jnp.mean(values, axis=-1, keepdims=True)
    row_var = jnp.mean(values * values, axis=-1, keepdims=True) - row_mean * row_mean
    return (values - row_mean) * lax.rsqrt(row_var + NORM_EPS) * gain_vec


def tile_of(size, want):
    tile = min(size, want)
    while size % tile:
        tile //= 2
    return tile


def normalise_tile(n_blocks, *refs):
    x_refs, gain_refs, out_refs = refs[:n_blocks], refs[n_blocks:2 * n_blocks], refs[-n_blocks:]
    full_width = n_blocks * x_refs[0].shape[1]
    total, squares = 0.0, 0.0
    for x_ref in x_refs:
        values = x_ref[...].astype(jnp.float32)
        total = total + jnp.sum(values, axis=-1, keepdims=True)
        squares = squares + jnp.sum(values * values, axis=-1, keepdims=True)
    row_mean = total / full_width
    row_var = squares / full_width - row_mean * row_mean
    inv = lax.rsqrt(row_var + NORM_EPS)
    for x_ref, gain_ref, out_ref in zip(x_refs, gain_refs, out_refs):
        out_ref[...] = ((x_ref[...].astype(jnp.float32) - row_mean) * inv * gain_ref[...]).astype(jnp.bfloat16)


def normalise(x_list, gain_list, held):
    rows, depth = x_list[0].shape
    n_blocks = len(x_list)
    bm = tile_of(rows, 64)
    steps = rows // bm
    shift = steps if held else 0
    row_block = pl.BlockSpec((bm, depth), lambda i: (i, 0))
    held = list(held or [])
    return pl.pallas_call(
        functools.partial(normalise_tile, n_blocks),
        out_shape=[jax.ShapeDtypeStruct((2 * rows, depth), jnp.bfloat16)] * n_blocks,
        grid=(steps,),
        in_specs=[row_block] * n_blocks + [pl.BlockSpec((1, depth), lambda i: (0, 0))] * n_blocks
        + [pl.BlockSpec(memory_space=pl.ANY)] * len(held),
        out_specs=[pl.BlockSpec((bm, depth), lambda i: (i + shift, 0))] * n_blocks,
        input_output_aliases={2 * n_blocks + k: k for k in range(len(held))},
        compiler_params=pltpu.CompilerParams(vmem_limit_bytes=VMEM_LIMIT),
        cost_estimate=pl.CostEstimate(flops=600 * rows * depth * n_blocks, bytes_accessed=4 * rows * depth * n_blocks, transcendentals=0),
    )(*x_list, *[g.reshape(1, depth) for g in gain_list], *held)


def lane_tile(cols):
    return 256 if cols % 256 == 0 else 128


def block_matmul(n_blocks, with_gelu, *refs):
    n_refs, w_refs = refs[:n_blocks], refs[n_blocks:2 * n_blocks]
    out_ref = refs[-1]
    tile = lane_tile(out_ref.shape[1])

    def step(t, carry):
        cols = pl.ds(pl.multiple_of(t * tile, tile), tile)
        acc = jnp.dot(n_refs[0][...], w_refs[0][:, cols], preferred_element_type=jnp.float32)
        for n_ref, w_ref in zip(n_refs[1:], w_refs[1:]):
            acc = acc + jnp.dot(n_ref[...], w_ref[:, cols], preferred_element_type=jnp.float32)
        out = acc.astype(jnp.bfloat16)
        if with_gelu:
            bias = refs[2 * n_blocks][:, cols]
            out = jax.nn.gelu(out.astype(jnp.float32) + bias, approximate=True).astype(jnp.bfloat16)
        out_ref[:, cols] = out
        return carry

    lax.fori_loop(0, out_ref.shape[1] // tile, step, 0)


def project_in(n_list, w_list, bias, half=None, held=None):
    rows, depth = n_list[0].shape
    cols = w_list[0].shape[1]
    n_blocks = len(n_list)
    bm, bn = tile_of(rows // 2, 256), 768 if cols % 768 == 0 else tile_of(cols, 512)
    steps = rows // bm if half is None else rows // bm // 2
    shift = steps if half else 0
    in_specs = [pl.BlockSpec((bm, depth), lambda j, i: (i + shift, 0))] * n_blocks
    in_specs += [pl.BlockSpec((depth, bn), lambda j, i: (0, j))] * n_blocks
    operands = [*n_list, *w_list]
    if bias is not None:
        in_specs.append(pl.BlockSpec((1, bn), lambda j, i: (0, j)))
        operands.append(bias.reshape(1, cols))
    aliases = {}
    if held is not None:
        in_specs.append(pl.BlockSpec(memory_space=pl.ANY))
        aliases = {len(operands): 0}
        operands.append(held)
    flops = 2 * bm * steps * depth * n_blocks * cols
    return pl.pallas_call(
        functools.partial(block_matmul, n_blocks, bias is not None),
        out_shape=jax.ShapeDtypeStruct((rows, cols), jnp.bfloat16),
        grid=(cols // bn, steps),
        in_specs=in_specs,
        out_specs=pl.BlockSpec((bm, bn), lambda j, i: (i + shift, j)),
        input_output_aliases=aliases,
        compiler_params=pltpu.CompilerParams(vmem_limit_bytes=VMEM_LIMIT),
        cost_estimate=pl.CostEstimate(flops=flops, bytes_accessed=4 * n_blocks * depth * (rows + cols), transcendentals=0),
    )(*operands)


def out_matmul(n_hidden, n_adds, n_parts, has_res, *refs):
    out_ref = refs[-1]
    hidden_refs, w_ref = refs[:n_hidden], refs[n_hidden]
    rest = refs[n_hidden + 1:-1]
    tile = lane_tile(out_ref.shape[1])

    def step(t, carry):
        cols = pl.ds(pl.multiple_of(t * tile, tile), tile)
        acc, start = None, 0
        for h_ref in hidden_refs:
            stop = start + h_ref.shape[1]
            term = jnp.dot(h_ref[...], w_ref[start:stop, cols], preferred_element_type=jnp.float32)
            acc = term if acc is None else acc + term
            start = stop
        for add_ref in rest[:n_adds]:
            acc = acc + add_ref[:, cols].astype(jnp.float32)
        if has_res:
            acc = rest[n_adds + n_parts][:, cols].astype(jnp.float32) + acc + rest[n_adds + n_parts + 1][:, cols]
        out_ref[:, cols] = acc.astype(out_ref.dtype)
        return carry

    lax.fori_loop(0, out_ref.shape[1] // tile, step, 0)
    start = 0
    for part_ref in rest[n_adds:n_adds + n_parts]:
        stop = start + part_ref.shape[1]
        out_ref[:, start:stop] = out_ref[:, start:stop] + part_ref[...].astype(jnp.float32)
        start = stop


def project_out(hidden, w, adds, half=None, parts=(), residual=None, bias=None, window=(0, 1)):
    all_rows = hidden[0].shape[0]
    rows = all_rows if half is None else all_rows // 2
    index, count = window
    depth, cols = w.shape[0], w.shape[1] // count
    bm = tile_of(rows, 512)

    def row_block(arr, width, col_index=0):
        shift = rows // bm if half and arr.shape[0] == all_rows else 0
        return pl.BlockSpec((bm, width), lambda i: (i + shift, col_index))

    in_specs = [row_block(h, h.shape[1]) for h in hidden] + [pl.BlockSpec((depth, cols), lambda i: (0, index))]
    in_specs += [row_block(a, cols, index) for a in adds]
    in_specs += [row_block(p, p.shape[1]) for p in parts]
    operands = [*hidden, w, *adds, *parts]
    out_type = jnp.bfloat16
    if residual is not None:
        in_specs += [row_block(residual, cols), pl.BlockSpec((1, cols), lambda i: (0, 0))]
        operands += [residual, bias.reshape(1, cols)]
        out_type = jnp.float32
    return pl.pallas_call(
        functools.partial(out_matmul, len(hidden), len(adds), len(parts), residual is not None),
        out_shape=jax.ShapeDtypeStruct((rows, cols), out_type),
        grid=(rows // bm,),
        in_specs=in_specs,
        out_specs=pl.BlockSpec((bm, cols), lambda i: (i, 0)),
        compiler_params=pltpu.CompilerParams(vmem_limit_bytes=VMEM_LIMIT),
        cost_estimate=pl.CostEstimate(flops=2 * rows * depth * cols, bytes_accessed=2 * (rows + cols) * depth, transcendentals=0),
    )(*operands)


def add_parts(main_ref, *refs):
    out_ref, start = refs[-1], 0
    for part_ref in refs[:-1]:
        stop = start + part_ref.shape[1]
        out_ref[:, start:stop] = (main_ref[:, start:stop] + part_ref[...].astype(jnp.float32)).astype(out_ref.dtype)
        start = stop


def add_last(main_ref, part_ref, held_ref, out_ref):
    out_ref[...] = (main_ref[...] + part_ref[...].astype(jnp.float32)).astype(out_ref.dtype)


def join_parts(main, parts):
    rows, cols = main.shape
    bm = tile_of(rows, 128)
    row_block = lambda width: pl.BlockSpec((bm, width), lambda i: (i, 0))
    return pl.pallas_call(
        add_parts,
        out_shape=jax.ShapeDtypeStruct((rows, cols), jnp.bfloat16),
        grid=(rows // bm,),
        in_specs=[row_block(cols)] + [row_block(p.shape[1]) for p in parts],
        out_specs=row_block(cols),
        compiler_params=pltpu.CompilerParams(vmem_limit_bytes=SMALL_LIMIT),
        cost_estimate=pl.CostEstimate(flops=2 * rows * cols, bytes_accessed=8 * rows * cols, transcendentals=0),
    )(main, *parts)


def join_last(main, part, held):
    rows, cols = main.shape
    size = part.shape[1]
    bm = tile_of(rows, 1024)
    last = cols // size - 1
    tail_block = pl.BlockSpec((bm, size), lambda i: (i, last))
    return pl.pallas_call(
        add_last,
        out_shape=jax.ShapeDtypeStruct((rows, cols), jnp.bfloat16),
        grid=(rows // bm,),
        in_specs=[tail_block, pl.BlockSpec((bm, size), lambda i: (i, 0)), pl.BlockSpec(memory_space=pl.ANY)],
        out_specs=tail_block,
        input_output_aliases={2: 0},
        compiler_params=pltpu.CompilerParams(vmem_limit_bytes=SMALL_LIMIT),
        cost_estimate=pl.CostEstimate(flops=2 * rows * size, bytes_accessed=8 * rows * size, transcendentals=0),
    )(main, part, held)


def attend(head_dim, qs_ref, ks_ref, *refs):
    out_ref, done = refs[-1], 0
    for qkv_ref in refs[:-1]:
        for base in range(0, qkv_ref.shape[1], 3 * head_dim):
            q = layer_norm_rows(qkv_ref[:, base:base + head_dim].astype(jnp.float32), qs_ref[...]).astype(jnp.bfloat16)
            k = layer_norm_rows(qkv_ref[:, base + head_dim:base + 2 * head_dim].astype(jnp.float32), ks_ref[...]).astype(jnp.bfloat16)
            v = qkv_ref[:, base + 2 * head_dim:base + 3 * head_dim]
            s = lax.dot_general(q, k, (((1,), (1,)), ((), ())), preferred_element_type=jnp.float32) * head_dim ** -0.5
            e = jnp.exp(s - jnp.max(s, axis=-1, keepdims=True))
            p = (e / jnp.sum(e, axis=-1, keepdims=True)).astype(jnp.bfloat16)
            out_ref[:, done:done + head_dim] = jnp.dot(p, v, preferred_element_type=jnp.float32).astype(jnp.bfloat16)
            done += head_dim


def attention(qkv_list, q_scale, k_scale, seq_len):
    rows = qkv_list[0].shape[0]
    widths = [q.shape[1] for q in qkv_list]
    head_dim = q_scale.shape[0]
    out_width = sum(widths) // 3
    scale_spec = pl.BlockSpec((1, head_dim), lambda i: (0, 0))
    flops = 4 * rows * seq_len * out_width
    return pl.pallas_call(
        functools.partial(attend, head_dim),
        out_shape=jax.ShapeDtypeStruct((rows, out_width), jnp.bfloat16),
        grid=(rows // seq_len,),
        in_specs=[scale_spec, scale_spec] + [pl.BlockSpec((seq_len, w), lambda i: (i, 0)) for w in widths],
        out_specs=pl.BlockSpec((seq_len, out_width), lambda i: (i, 0)),
        compiler_params=pltpu.CompilerParams(vmem_limit_bytes=VMEM_LIMIT),
        cost_estimate=pl.CostEstimate(flops=8 * flops, bytes_accessed=2 * rows * sum(widths), transcendentals=0),
    )(q_scale.reshape(1, head_dim), k_scale.reshape(1, head_dim), *qkv_list)


def solution(mesh):
    col_size = mesh.shape['col']
    row_size = mesh.shape['row']

    def partner(arr, shift):
        return lax.ppermute(arr, 'col', [(i, i ^ shift) for i in range(col_size)])

    def over_row(arr):
        return lax.ppermute(arr, 'row', [(i, i ^ 1) for i in range(row_size)])

    def layer(x_loc, ln_scale, w_qkv, q_scale, k_scale, w_out, w_up, b_up, w_down, b_down):
        col = lax.axis_index('col')
        imgs, seq_len, width = x_loc.shape
        x_rows = x_loc.reshape(imgs * seq_len, width)

        def piece_cols(w, shift, start, size):
            span = w.shape[1] // col_size
            return lax.dynamic_slice(w, (0, (col ^ shift) * span + start), (w.shape[0], size))

        def piece_rows(w, shift, start, size):
            span = w.shape[0] // col_size
            return lax.dynamic_slice(w, ((col ^ shift) * span, start), (span, size))

        def in_weights(w, start, size):
            return [piece_cols(w, 0, start, size)] + [
                partner(piece_cols(w, s, start, size), s) for s in (1, 2, 3)]

        def out_piece(shift, start, size):
            return jnp.concatenate([piece_rows(w_out, shift, start, size), piece_rows(w_down, shift, start, size)], axis=0)

        gains = [ln_scale] + [partner(ln_scale, s) for s in (1, 2, 3)]
        x1 = partner(x_rows, 1)
        x2 = partner(x_rows, 2)
        z0 = over_row(x_rows)
        x3 = partner(x2, 1)
        z2 = over_row(x2)
        z1 = partner(z0, 1)
        z3 = partner(z2, 1)
        first = normalise([x_rows, x1, x2, x3], gains, None)
        both = normalise([z0, z1, z2, z3], gains, first)

        head_cols = 3 * q_scale.shape[0]
        qkv_cols = w_qkv.shape[1] // col_size
        up_cols = w_up.shape[1] // col_size
        qkv_step, up_step = 2 * head_cols, up_cols // UP_PIECES
        qkv, hidden = [], []
        for i in range(qkv_cols // qkv_step):
            w = in_weights(w_qkv, i * qkv_step, qkv_step)
            if i < EARLY:
                part = project_in(first, w, None, half=0)
                qkv.append(project_in(both, w, None, half=1, held=part))
            else:
                qkv.append(project_in(both, w, None))
        hidden.append(attention(qkv, q_scale, k_scale, seq_len))
        for i in range(UP_PIECES):
            w = in_weights(w_up, i * up_step, up_step)
            bias = lax.dynamic_slice(b_up, (col * up_cols + i * up_step,), (up_step,))
            if i < UP_PIECES - 1:
                hidden.append(project_in(both, w, bias))
        up_oth = project_in(both, w, bias, half=1)
        up_both = project_in(both, w, bias, half=0, held=up_oth)
        hid_oth, hid = [*hidden, up_oth], [*hidden, up_both]

        out_cols = w_out.shape[1]
        wo_0 = out_piece(0, 0, out_cols)
        wo_1 = partner(out_piece(1, 0, out_cols), 1)
        d1_oth = partner(project_out(hid_oth, wo_1, [], half=1), 1)
        d1_own = partner(project_out(hid, wo_1, [], half=0), 1)
        y0 = [over_row(project_out(hid, wo_0, [d1_oth], half=1, window=(i, Y_PIECES))) for i in range(Y_PIECES)]
        x_parts, start = [], 0
        for size in OUT_PIECES:
            wo_3 = partner(out_piece(3, start, size), 3)
            wo_2 = partner(out_piece(2, start, size), 2)
            d3 = partner(project_out(hid, wo_3, []), 1)
            y2 = over_row(project_out(hid, wo_2, [d3], half=1))
            x_parts.append(partner(project_out(hid, wo_2, [d3, y2], half=0), 2))
            start += size
        main = project_out(hid, wo_0, [d1_own], half=0, parts=y0, residual=x_rows, bias=b_down)
        out = join_last(main, x_parts[-1], join_parts(main, x_parts[:-1]))
        return out.reshape(imgs, seq_len, width)

    x_spec = P(('dp', 'row'), None, 'col')
    return jax.shard_map(layer, mesh=mesh,
                         in_specs=(x_spec, P('col'), P('col', 'row'), P(), P(), P('row', 'col'), P('col', 'row'), P('row'), P('row', 'col'), P('col')),
                         out_specs=x_spec, check_vma=False)
```
